32 devices in a mesh: groups: 2 (over y), tile: 4 (over z), face: 4 (over x, core).
Axes of the slice: x: 2, y: 2, z: 4, core: 2. Of those that a mesh axis runs over, the one named last changes fastest.
Arguments:
- noisy_state: float32 [24, 256, 512], P('groups', 'face', 'tile'), parts along dimension 0, may hold values from -6 to 6
- conditioning: float32 [24, 256, 512], P('groups', 'face', 'tile'), parts along dimension 0, may hold values from -6 to 6
- orient: int32 [4, 8], replicated, may hold values from 0 to 3
- corner_points: int32 [4, 8], replicated, may hold values 0 or 1
- w_state: bfloat16 [128, 108], replicated, may hold values from -0.625 to 0.625
- w_cond: bfloat16 [128, 108], replicated, may hold values from -0.625 to 0.625
- w_out: bfloat16 [108, 128], replicated, may hold values from -0.1875 to 0.1875
- embed_first: float32 [128], replicated, may hold values from -3 to 3
- embed_second: float32 [128], replicated, may hold values from -3 to 3
Outputs:
- next_state: float32 [24, 256, 512], P('groups', 'face', 'tile'), parts along dimension 0
The draws below stay inside these ranges and needn't reach their ends.
There are 2 independent parts, one for each index of `groups`. The reference program is written for one: setup_inputs(seed, part) draws one part's arguments, and reference() takes and returns one part's arrays. A program takes and returns all parts, laid end to end along the dimension named above; an argument that names none is the same for every part. Nothing has to cross between parts.
Inputs may be any that keep to these rules, and one draw needn't show every extreme that they name: `orient`: A tile's stored pixels are its pixels in the grid's frame turned by this many quarter turns. `corner_points`: entry (r, c) belongs to the upper-left corner of tile (r, c).
All inputs are finite; a program needn't handle non-finite values.
Results may differ from the reference program's by a relative error of at most 0.0019.
Values sent between devices are 32-bit elements; how exact they have to be, the bound alone decides.
No kernel may reach another device: no remote copies, remote signals or barrier semaphores. Data moves between devices by JAX's collectives and lax.ppermute only.
A program may use at most 256 MiB of HBM per device.

```python
import math
import jax
import jax.numpy as jnp
from jax import lax

FIELDS = 12
HIDDEN_SIZE = 128
P_SIZE = 64
RIM = 8
NR = 4
NC = 8
ROWS = 256
COLS = 512


def with_ends(result, key, smallest, largest):
    place = [jax.random.randint(jax.random.fold_in(key, axis), (), 0, length) for axis, length in enumerate(result.shape)]
    main_axis = result.shape.index(max(result.shape))
    beside = place[:main_axis] + [(place[main_axis] + 1) % result.shape[main_axis]] + place[main_axis + 1:]
    return result.at[tuple(place)].set(smallest).at[tuple(beside)].set(largest)


def block_levels(own_key, shape, cuts, least, high):
    factor_of = 1.0
    for dim, blocks in cuts:
        draws = jax.random.uniform(jax.random.fold_in(jax.random.fold_in(own_key, 6), dim), (blocks,), jnp.float32, least / len(cuts), high / len(cuts))
        factor_of = factor_of * jnp.repeat(jnp.exp(draws), shape[dim] // blocks).reshape((-1,) + (1,) * (len(shape) - 1 - dim))
    return factor_of


def centred(stream_key, shape, scale, most, split=(), kind=jnp.bfloat16):
    drawn = jax.random.normal(stream_key, shape, jnp.float32) * scale
    if len(split) > 0:
        drawn = block_levels(stream_key, shape, split, -0.22, 0.18) * drawn
    return jnp.clip(drawn, min=-most, max=most).astype(kind)


def setup_inputs(seed: int = 0, part: int = 0) -> dict:
    seeds = jax.random.split(jax.random.key(seed), 10)
    own_keys = jax.random.split(jax.random.fold_in(seeds[9], part), 10)
    return {
        "noisy_state": centred(own_keys[0], (FIELDS, ROWS, COLS), 1.0, 6.0, ((1, 4), (2, 4)), jnp.float32),
        "conditioning": centred(own_keys[1], (FIELDS, ROWS, COLS), 1.0, 6.0, ((1, 4), (2, 4)), jnp.float32),
        "orient": with_ends(jax.random.randint(seeds[2], (NR, NC), 0, 4), jax.random.fold_in(seeds[2], 1), 0, 3).astype(jnp.int32),
        "corner_points": with_ends((jax.random.randint(seeds[3], (NR, NC), 0, 8) < 1).astype(jnp.int32), jax.random.fold_in(seeds[3], 1), 0, 1),
        "w_state": centred(seeds[4], (HIDDEN_SIZE, 9 * FIELDS), (9 * FIELDS) ** -0.5, 0.625),
        "w_cond": centred(seeds[5], (HIDDEN_SIZE, 9 * FIELDS), (9 * FIELDS) ** -0.5, 0.625),
        "w_out": centred(seeds[6], (9 * FIELDS, HIDDEN_SIZE), (9 * HIDDEN_SIZE) ** -0.5, 0.1875),
        "embed_first": centred(seeds[7], (HIDDEN_SIZE,), 0.5, 3.0, (), jnp.float32),
        "embed_second": centred(seeds[8], (HIDDEN_SIZE,), 0.5, 3.0, (), jnp.float32),
    }


guide_weight = 2.0
sigma_first = 1.0
sigma_second = 0.6
step_size = sigma_second - sigma_first
scale_first = 1.0 / math.sqrt(1.0 + sigma_first ** 2)
scale_second = 1.0 / math.sqrt(1.0 + sigma_second ** 2)

def rotate_by(picture, quarters):
    turned = jnp.stack([jnp.rot90(picture, quarter, axes=(-2, -1)) for quarter in range(4)])
    return turned[quarters]

def patches(picture):
    channels, height, breadth = picture.shape
    padded = jnp.pad(picture, ((0, 0), (1, 1), (1, 1)))
    stacked = jnp.concatenate([padded[:, row_step:row_step + height, col_step:col_step + breadth] for row_step in range(3) for col_step in range(3)], axis=0)
    return stacked.reshape(9 * channels, height * breadth)

def spread(products, channels, height, breadth):
    shaped = products.reshape(9, channels, height, breadth)
    padded = jnp.pad(shaped, ((0, 0), (0, 0), (1, 1), (1, 1)))
    summed = jnp.zeros((channels, height, breadth), jnp.float32)
    for row_step in range(3):
        for col_step in range(3):
            summed = summed + padded[3 * row_step + col_step, :, row_step:row_step + height, col_step:col_step + breadth]
    return summed

def predict(own_frame, feature, w_state, w_out, embedding, input_scale):
    channels, height, breadth = own_frame.shape
    lowered = (input_scale * own_frame).astype(jnp.bfloat16)
    mixed_sum = jnp.dot(w_state, patches(lowered), preferred_element_type=jnp.float32) + embedding[:, None]
    plain_hidden = jax.nn.silu(mixed_sum).astype(jnp.bfloat16)
    cond_hidden = jax.nn.silu(mixed_sum + feature).astype(jnp.bfloat16)
    plain_prod = jnp.dot(w_out, plain_hidden, preferred_element_type=jnp.float32)
    cond_prod = jnp.dot(w_out, cond_hidden, preferred_element_type=jnp.float32)
    return spread(plain_prod + guide_weight * (cond_prod - plain_prod), channels, height, breadth)

def corner_flags(corner_points, tile_row, tile_col):
    grid_rows, grid_cols = corner_points.shape
    next_row = (tile_row + 1) % grid_rows
    next_col = (tile_col + 1) % grid_cols
    return (corner_points[tile_row, tile_col], corner_points[tile_row, next_col], corner_points[next_row, tile_col], corner_points[next_row, next_col])

def corner_keep(corner_cut, tile_side):
    extent = tile_side + 2 * RIM
    row_ids = jnp.arange(extent, dtype=jnp.int32)[:, None]
    col_ids = jnp.arange(extent, dtype=jnp.int32)[None, :]
    upper_band = row_ids < RIM
    lower_band = row_ids >= tile_side + RIM
    left_side = col_ids < RIM
    right_side = col_ids >= tile_side + RIM
    dropped = upper_band & left_side & (corner_cut[0] == 1) | upper_band & right_side & (corner_cut[1] == 1) | lower_band & left_side & (corner_cut[2] == 1) | lower_band & right_side & (corner_cut[3] == 1)
    return jnp.where(dropped, 0.0, 1.0).astype(jnp.float32)

def coverage_of(local_row, local_col, corner_cut, tile_side):
    upper_band = local_row < RIM
    lower_band = local_row >= tile_side - RIM
    left_side = local_col < RIM
    right_side = local_col >= tile_side - RIM
    edge_hits = upper_band.astype(jnp.float32) + lower_band.astype(jnp.float32) + left_side.astype(jnp.float32) + right_side.astype(jnp.float32)
    diagonal = (upper_band & left_side & (corner_cut[0] == 0)).astype(jnp.float32)
    diagonal = diagonal + (upper_band & right_side & (corner_cut[1] == 0)).astype(jnp.float32)
    diagonal = diagonal + (lower_band & left_side & (corner_cut[2] == 0)).astype(jnp.float32)
    diagonal = diagonal + (lower_band & right_side & (corner_cut[3] == 0)).astype(jnp.float32)
    return 1.0 + edge_hits + diagonal

def reframe(field_data, turn_codes):
    fields = field_data.shape[0]
    blocks = field_data.reshape(fields, NR, P_SIZE, NC, P_SIZE).transpose(1, 3, 0, 2, 4).reshape(NR * NC, fields, P_SIZE, P_SIZE)

    def turn_one(pieces):
        return rotate_by(pieces[0], pieces[1])
    turned = lax.map(turn_one, (blocks, turn_codes.reshape(-1)))
    return turned.reshape(NR, NC, fields, P_SIZE, P_SIZE).transpose(2, 0, 3, 1, 4).reshape(fields, NR * P_SIZE, NC * P_SIZE)

def fold_back(running):
    middle = running[:, :, RIM:-RIM]
    middle = middle.at[:, :, :RIM].add(running[:, :, -RIM:])
    middle = middle.at[:, :, -RIM:].add(running[:, :, :RIM])
    interior = middle[:, RIM:-RIM]
    interior = interior.at[:, :RIM].add(middle[:, -RIM:])
    interior = interior.at[:, -RIM:].add(middle[:, :RIM])
    return interior

def evaluate(glob_field, cond_padded, orient, corner_points, w_state, w_cond, w_out, embedding, input_scale):
    fields = glob_field.shape[0]
    extent = P_SIZE + 2 * RIM
    padded = jnp.pad(glob_field, ((0, 0), (RIM, RIM), (RIM, RIM)), mode='wrap')

    def one_tile(running, tile_index):
        tile_row = tile_index // NC
        tile_col = tile_index % NC
        corner_cut = corner_flags(corner_points, tile_row, tile_col)
        keep_mask = corner_keep(corner_cut, P_SIZE)
        offsets = (jnp.zeros((), jnp.int32), (tile_row * P_SIZE).astype(jnp.int32), (tile_col * P_SIZE).astype(jnp.int32))
        window = lax.dynamic_slice(padded, offsets, (fields, extent, extent)) * keep_mask
        cond_window = lax.dynamic_slice(cond_padded, offsets, (fields, extent, extent)) * keep_mask
        turn_code = orient[tile_row, tile_col]
        own_cond = rotate_by(cond_window, turn_code).astype(jnp.bfloat16)
        feature = jnp.dot(w_cond, patches(own_cond), preferred_element_type=jnp.float32)
        guided = predict(rotate_by(window, turn_code), feature, w_state, w_out, embedding, input_scale)
        returned = rotate_by(guided, (4 - turn_code) % 4) * keep_mask
        current = lax.dynamic_slice(running, offsets, (fields, extent, extent))
        return (lax.dynamic_update_slice(running, current + returned, offsets), None)
    running = jnp.zeros((fields, ROWS + 2 * RIM, COLS + 2 * RIM), jnp.float32)
    running, unused = lax.scan(one_tile, running, jnp.arange(NR * NC, dtype=jnp.int32))
    total = fold_back(running)
    row_ids = jnp.arange(ROWS, dtype=jnp.int32)[:, None]
    col_ids = jnp.arange(COLS, dtype=jnp.int32)[None, :]
    corner_cut = corner_flags(corner_points, row_ids // P_SIZE, col_ids // P_SIZE)
    coverage = coverage_of(row_ids % P_SIZE, col_ids % P_SIZE, corner_cut, P_SIZE)
    return total / coverage[None]

def reference(noisy_state, conditioning, orient, corner_points, w_state, w_cond, w_out, embed_first, embed_second):
    to_global = (4 - orient) % 4
    glob_state = reframe(noisy_state, to_global)
    glob_cond = reframe(conditioning, to_global)
    cond_padded = jnp.pad(glob_cond, ((0, 0), (RIM, RIM), (RIM, RIM)), mode='wrap')
    slope_first = evaluate(glob_state, cond_padded, orient, corner_points, w_state, w_cond, w_out, embed_first, scale_first)
    middle = glob_state + step_size * slope_first
    slope_second = evaluate(middle, cond_padded, orient, corner_points, w_state, w_cond, w_out, embed_second, scale_second)
    updated = glob_state + 0.5 * step_size * (slope_first + slope_second)
    return reframe(updated, orient)
```

```python
import functools
import math

import numpy as np

import jax
import jax.numpy as jnp
from jax import lax
from jax.experimental import pallas as pl
from jax.experimental.pallas import tpu as pltpu
from jax.sharding import PartitionSpec as P

RIM = 8
REACH = 4
KBLOCK = 80
OUT = 16
ZROWS = 9 * OUT

guide_weight = 2.0
sigma_first = 1.0
sigma_second = 0.6
step_size = sigma_second - sigma_first
scale_first = 1.0 / math.sqrt(1.0 + sigma_first**2)
scale_second = 1.0 / math.sqrt(1.0 + sigma_second**2)

f32 = jnp.float32
bf16 = jnp.bfloat16


def iota(shape, dim):
    return lax.broadcasted_iota(jnp.int32, shape, dim)


def roll(value, shift):
    shift = shift % value.shape[1]
    return value if shift == 0 else pltpu.roll(value, shift, 1)


def turned(first, second, codes, side):
    lanes = 2 * side
    lane = iota((side, lanes), 1)
    left = lane < side
    code = jnp.where(left, codes[0], codes[1])
    odd = (code & 1) == 1
    flip_rows = (code == 1) | (code == 2)
    flip_cols = code >= 2
    mirrored = jnp.where(left, side - 1 - lane, 3 * side - 1 - lane)
    index = jnp.where(flip_cols, mirrored, lane)
    both = jnp.concatenate([first, second], axis=0).T
    upper, lower = both[:side], both[side:]
    swapped = (
        jnp.where(left, upper, roll(lower, side)),
        jnp.where(left, roll(upper, side), lower),
    )
    results = []
    down = 7 - iota((8, lanes), 0)
    for plain, flipped in zip((first, second), swapped):
        value = jnp.where(odd, flipped, plain)
        value = jnp.take_along_axis(value, index, axis=1)
        groups = side // 8
        reversed_rows = jnp.concatenate(
            [
                jnp.take_along_axis(value[8 * (groups - 1 - i) : 8 * (groups - i)], down, axis=0)
                for i in range(groups)
            ],
            axis=0,
        )
        results.append(jnp.where(flip_rows, reversed_rows, value))
    return results


def prepare_kernel(orient_ref, state_ref, cond_ref, grid_ref, to_left_ref, to_right_ref):
    fields, side, lanes = state_ref.shape
    count = lanes // side
    both = 2 * fields
    tile_row = lax.axis_index("face")
    base = lax.axis_index("tile") * count
    codes = [(4 - orient_ref[tile_row, base + p]) & 3 for p in range(count)]
    for c in range(fields):
        a, b = turned(state_ref[c], cond_ref[c], codes, side)
        grid_ref[pl.ds(c, side, stride=both), :] = a
        grid_ref[pl.ds(fields + c, side, stride=both), :] = b
    lane_block = iota((both, lanes), 1) // REACH
    blocks = lanes // REACH
    per = side // blocks
    for j in range(per):
        to_left = jnp.zeros((both, lanes), f32)
        to_right = jnp.zeros((both, lanes), f32)
        for k in range(blocks):
            row = grid_ref[(per * k + j) * both : (per * k + j + 1) * both, :]
            here = lane_block == k
            to_left = jnp.where(here, roll(row, REACH * k), to_left)
            to_right = jnp.where(here, roll(row, REACH * k - (lanes - REACH)), to_right)
        to_left_ref[j * both : (j + 1) * both, :] = to_left
        to_right_ref[j * both : (j + 1) * both, :] = to_right


def prepare(orient, state, cond):
    fields, side, lanes = state.shape
    both = 2 * fields
    per = side // (lanes // REACH)
    vmem = pl.BlockSpec(memory_space=pltpu.VMEM)
    return pl.pallas_call(
        prepare_kernel,
        out_shape=(
            jax.ShapeDtypeStruct((side * both, lanes), f32),
            jax.ShapeDtypeStruct((per * both, lanes), f32),
            jax.ShapeDtypeStruct((per * both, lanes), f32),
        ),
        in_specs=[pl.BlockSpec(memory_space=pltpu.SMEM), vmem, vmem],
        out_specs=(vmem, vmem, vmem),
        name="prepare",
    )(orient, state, cond)


def edges_kernel(top_ref, bottom_ref, left_ref, right_ref, up_ref, down_ref):
    rows, lanes = top_ref.shape
    half = lanes // 2
    near = iota(left_ref.shape, 1) < half
    left, right = left_ref[...], roll(right_ref[...], half)
    up_ref[:rows] = top_ref[...]
    up_ref[rows:] = jnp.where(near, left, right)
    down_ref[:rows] = bottom_ref[...]
    down_ref[rows:] = jnp.where(near, right, left)


def edges(grid, left, right, both):
    total, lanes = grid.shape
    rows = REACH * both
    extra = left.shape[0]
    last = total // rows - 1
    whole = pl.BlockSpec((extra, lanes), lambda i: (0, 0))
    sent = pl.BlockSpec((rows + extra, lanes), lambda i: (0, 0))
    return pl.pallas_call(
        edges_kernel,
        grid=(1,),
        out_shape=(jax.ShapeDtypeStruct((rows + extra, lanes), f32),) * 2,
        in_specs=[
            pl.BlockSpec((rows, lanes), lambda i: (0, 0)),
            pl.BlockSpec((rows, lanes), lambda i: (last, 0)),
            whole,
            whole,
        ],
        out_specs=(sent, sent),
        name="edges",
    )(grid, grid, left, right)


def grid_taps(code):
    return np.rot90(np.arange(9).reshape(3, 3), (4 - code) % 4)


def selections(fields):
    state_sel = np.zeros((4, 9 * fields, 256), np.float32)
    cond_sel = np.zeros((4, 9 * fields, 256), np.float32)
    out_sel = np.zeros((4, ZROWS, 9 * fields), np.float32)
    for code in range(4):
        taps = grid_taps(code)
        for a in range(3):
            for b in range(3):
                for c in range(fields):
                    source = taps[a, b] * fields + c
                    target = a * KBLOCK + b * 2 * fields + c
                    state_sel[code, source, target] = 1.0
                    cond_sel[code, source, target + fields] = 1.0
                    out_sel[code, (3 * a + b) * OUT + c, source] = 1.0
    return state_sel, cond_sel, out_sel


class Plan:
    def __init__(self, side, lanes):
        self.side, self.lanes = side, lanes
        self.count = lanes // side
        self.ext = side + 2 * REACH
        self.extent = side + 2 * RIM
        self.strip = REACH + RIM
        self.block_lanes = self.strip + 2
        self.long_blocks = lanes // self.block_lanes
        outs = side + REACH
        self.long_rows = -(-outs // self.long_blocks)
        short = RIM + REACH // 2
        self.short_rows = 2
        self.short_blocks = short // self.short_rows
        self.units = []
        for p in range(self.count):
            self.units.append(("mid", p, self.ext - 2))
        for p in range(self.count):
            self.units.append(("up", p, self.strip))
            self.units.append(("down", p, self.strip))
        for s in ("left", "right"):
            self.units.append((s, None, self.long_rows + 2))
        for s in ("up_left", "up_right", "down_left", "down_right"):
            self.units.append((s, None, self.short_rows + 2))
        self.x0, self.z0, self.unit_of = [], [], []
        x = z = 0
        for i, (_, _, hidden) in enumerate(self.units):
            assert hidden % 2 == 0
            self.x0.append(x)
            self.z0.append(z)
            x += hidden + 2
            z += hidden
            self.unit_of += [i] * (hidden // 2)
        self.x_rows, self.z_rows = x, z
        self.pairs = len(self.unit_of)

    def at(self, name, p=None):
        for i, (n, q, _) in enumerate(self.units):
            if n == name and q == p:
                return i


def main_kernel(
    plan,
    sizes,
    unit_of_ref,
    orient_ref,
    corner_ref,
    state_ref,
    grid_ref,
    left_ref,
    right_ref,
    up_ref,
    down_ref,
    w_state_ref,
    w_cond_ref,
    w_out_ref,
    embed_ref,
    sel_state_ref,
    sel_cond_ref,
    sel_out_ref,
    out_ref,
    frame_ref,
    total_ref,
    slope_ref,
    x_ref,
    z_ref,
    w_ref,
    wo_ref,
    code_ref,
):
    fields, side, lanes = state_ref.shape
    both = 2 * fields
    count, ext, extent, strip = plan.count, plan.ext, plan.extent, plan.strip
    n_rows, n_cols = sizes
    tile_row = lax.axis_index("face")
    base = lax.axis_index("tile") * count

    def code_at(dr, dc):
        row = lax.rem(tile_row + dr + n_rows, n_rows)
        col = lax.rem(base + dc + n_cols, n_cols)
        return orient_ref[row, col]

    def flag_at(dr, dc):
        row = lax.rem(tile_row + dr, n_rows)
        col = lax.rem(base + dc, n_cols)
        return corner_ref[row, col].astype(f32)

    rows_of = {"mid": 0, "up": -1, "down": 1}
    for i, (name, p, _) in enumerate(plan.units):
        if p is not None:
            code_ref[i] = code_at(rows_of[name], p)
        else:
            dr = -1 if name.startswith("up") else (1 if name.startswith("down") else 0)
            dc = -1 if name.endswith("left") else count
            code_ref[i] = code_at(dr, dc)
    flags = [[flag_at(i, p) for p in range(count + 1)] for i in range(2)]

    lane24 = iota((both, lanes), 1)

    per = side // (lanes // REACH)

    def ext_row(e):
        if e < REACH:
            k, j = (side - REACH + e) // per, (side - REACH + e) % per
            source, row, half = up_ref, e, lanes // 2
            off = REACH * both
            return (
                source[row * both : (row + 1) * both, :],
                (source[off + j * both : off + (j + 1) * both, :], REACH * k),
                (source[off + j * both : off + (j + 1) * both, :], REACH * k - half),
            )
        if e >= ext - REACH:
            r = e - (ext - REACH)
            k, j = r // per, r % per
            off = REACH * both
            piece = down_ref[off + j * both : off + (j + 1) * both, :]
            return (
                down_ref[r * both : (r + 1) * both, :],
                (piece, REACH * k),
                (piece, REACH * k + lanes // 2),
            )
        r = e - REACH
        k, j = r // per, r % per
        return (
            grid_ref[r * both : (r + 1) * both, :],
            (left_ref[j * both : (j + 1) * both, :], REACH * k),
            (right_ref[j * both : (j + 1) * both, :], REACH * k),
        )

    for e in range(ext):
        row, left, right = ext_row(e)
        for p in range(count):
            value = roll(row, RIM - side * p)
            lo = max(0, RIM - side * p)
            hi = min(extent, lanes + RIM - side * p)
            value = jnp.where((lane24 >= lo) & (lane24 < hi), value, 0.0)
            if p == 0:
                here = (lane24 >= RIM - REACH) & (lane24 < RIM)
                value = jnp.where(here, roll(left[0], RIM - REACH - left[1]), value)
            if p == count - 1:
                here = (lane24 >= hi) & (lane24 < hi + REACH)
                value = jnp.where(here, roll(right[0], hi - right[1]), value)
            frame_ref[p, e * both : (e + 1) * both, :] = value

    hidden = w_state_ref.shape[0]
    embeds = []
    for ev in range(2):
        column = jnp.broadcast_to(embed_ref[ev : ev + 1, :], (hidden, hidden)).T * 0.5
        high = column.astype(bf16).astype(f32)
        middle = (column - high).astype(bf16).astype(f32)
        embeds.append((high, middle, column - high - middle))
    ones_at = KBLOCK + 6 * fields
    for code in range(4):
        from_state = jnp.dot(w_state_ref[...], sel_state_ref[code], preferred_element_type=f32) * 0.5
        from_cond = jnp.dot(w_cond_ref[...], sel_cond_ref[code], preferred_element_type=f32) * 0.5
        lane_w = iota(from_state.shape, 1)
        for ev in range(2):
            bias = jnp.zeros(from_state.shape, f32)
            for i, part in enumerate(embeds[ev]):
                wide = jnp.concatenate([part, part], axis=1)
                bias = jnp.where(lane_w == ones_at + i, wide, bias)
            w_ref[ev, code, :hidden, :] = (from_state + bias).astype(bf16)
            w_ref[ev, code, hidden:, :] = (from_state + from_cond + bias).astype(bf16)
        picked = jnp.dot(sel_out_ref[code], w_out_ref[...], preferred_element_type=f32)
        wo_ref[code] = jnp.concatenate(
            [picked * (1.0 - guide_weight), picked * guide_weight], axis=1
        ).astype(bf16)

    slope_ref[...] = jnp.zeros_like(slope_ref)
    x_ref[plan.x_rows * KBLOCK :, :] = jnp.zeros((256 - KBLOCK, lanes), bf16)

    lane1 = iota((1, lanes), 1)
    inside = (lane1 < extent).astype(f32)
    first8 = (lane1 < RIM).astype(f32)
    last8 = ((lane1 >= side + RIM) & (lane1 < extent)).astype(f32)

    def cut(left_flag, right_flag):
        return inside * (1.0 - left_flag * first8) * (1.0 - right_flag * last8)

    cuts = [[cut(flags[i][p], flags[i][p + 1]) for p in range(count)] for i in range(2)]
    last = count - 1
    left_lo = RIM - REACH
    right_lo = side
    left_cut8 = ((lane1 >= RIM) & (lane1 < 2 * RIM)).astype(f32)
    right_cut8 = ((lane1 >= side) & (lane1 < side + RIM)).astype(f32)
    left_in = ((lane1 >= left_lo) & (lane1 < left_lo + strip)).astype(f32)
    right_in = ((lane1 >= right_lo) & (lane1 < right_lo + strip)).astype(f32)
    left_out = ((lane1 >= RIM - 2) & (lane1 < 2 * RIM)).astype(f32)
    right_out = ((lane1 >= side) & (lane1 < side + RIM + 2)).astype(f32)

    def side_cut(right, flag):
        return 1.0 - flag * (right_cut8 if right else left_cut8)

    col_edge = first8 + ((lane1 >= RIM) & (lane1 < 2 * RIM)).astype(f32)
    col_edge_r = ((lane1 >= side) & (lane1 < side + 2 * RIM)).astype(f32)
    band = col_edge + col_edge_r
    cover_mid = 1.0 / (1.0 + band)
    cover_row = [
        [
            1.0 / (2.0 * (1.0 + band) - flags[i][p] * col_edge - flags[i][p + 1] * col_edge_r)
            for p in range(count)
        ]
        for i in range(2)
    ]

    spare = jnp.concatenate(
        [jnp.ones((KBLOCK - 6 * fields, lanes), f32)], axis=0
    )

    def put(row, value):
        stack = jnp.concatenate([roll(value, 1), value, roll(value, -1), spare], axis=0)
        x_ref[pl.ds(pl.multiple_of(row * KBLOCK, 16), KBLOCK), :] = stack.astype(bf16)

    def put_zero(row):
        x_ref[row * KBLOCK : (row + 1) * KBLOCK, :] = jnp.zeros((KBLOCK, lanes), bf16)

    def spread(z, m_first, m_last, terms=(None, None, None)):
        sums = []
        for b in range(3):
            parts = []
            for a in range(3):
                if isinstance(terms[a], int):
                    continue
                part = z_ref[z + a, (3 * a + b) * OUT : (3 * a + b + 1) * OUT, :]
                if terms[a] is not None:
                    part = part * terms[a]
                parts.append(part)
            sums.append(functools.reduce(jnp.add, parts))
        return sums[1] + roll(sums[0], 1) * m_first + roll(sums[2], -1) * m_last

    not_first = (lane1 != 0).astype(f32)
    not_last = (lane1 != extent - 1).astype(f32)
    phase = lane1 % plan.block_lanes
    block_of = lane1 // plan.block_lanes
    block_not_first = (phase != 0).astype(f32)
    block_not_last = (phase != strip - 1).astype(f32)
    nothing = jnp.ones((1, lanes), f32)

    def in_block(k):
        return (block_of == k) & (phase < strip)

    def evaluation(ev, carry):
        scale = jnp.where(ev == 0, f32(scale_first), f32(scale_second))
        scales = jnp.where(iota((both, lanes), 0) < fields, scale, 1.0)

        def frame(p, e):
            return frame_ref[p, pl.ds(pl.multiple_of(e * both, 8), both), :]

        for p in range(count):
            x0 = plan.x0[plan.at("mid", p)]
            top = scales * cuts[0][p]
            bottom = scales * cuts[1][p]
            plain = scales * inside
            for e in range(REACH):
                put(x0 + e, frame(p, e) * top)
                put(x0 + ext - REACH + e, frame(p, ext - REACH + e) * bottom)

            def mid_rows(e, c, p=p, x0=x0, plain=plain):
                put(x0 + e, frame(p, e) * plain)
                return c

            lax.fori_loop(REACH, ext - REACH, mid_rows, 0, unroll=8)
            x0 = plan.x0[plan.at("up", p)]
            for i in range(strip):
                put(x0 + i, frame(p, i) * (plain if i < REACH else top))
            put_zero(x0 + strip)
            put_zero(x0 + strip + 1)
            x0 = plan.x0[plan.at("down", p)]
            put_zero(x0)
            put_zero(x0 + 1)
            for i in range(strip):
                e = ext - strip + i
                put(x0 + 2 + i, frame(p, e) * (bottom if i < RIM else plain))

        for right in (False, True):
            p = last if right else 0
            lo = right_lo if right else left_lo
            inner = right_in if right else left_in
            vertex = count if right else 0
            plain = scales * inner
            top = plain * side_cut(right, flags[0][vertex])
            bottom = plain * side_cut(right, flags[1][vertex])
            x0 = plan.x0[plan.at("right" if right else "left")]
            for j in range(plan.long_rows + 4):
                value = jnp.zeros((both, lanes), f32)
                for k in range(plan.long_blocks):
                    e = plan.long_rows * k + j
                    if e >= ext:
                        continue
                    m = top if e < REACH else (bottom if e >= ext - REACH else plain)
                    piece = roll(frame(p, e) * m, plan.block_lanes * k - lo)
                    value = jnp.where(in_block(k), piece, value)
                put(x0 + j, value)
            for down in (False, True):
                flag = flags[1 if down else 0][vertex]
                marked = plain * side_cut(right, flag)
                name = ("down" if down else "up") + ("_right" if right else "_left")
                x0 = plan.x0[plan.at(name)]
                first = ext - strip - 2 if down else 0
                for j in range(plan.short_rows + 4):
                    value = jnp.zeros((both, lanes), f32)
                    for k in range(plan.short_blocks):
                        e = first + plan.short_rows * k + j
                        if down and e < ext - strip or not down and e >= strip:
                            continue
                        near = e < ext - REACH if down else e >= REACH
                        m = marked if near else plain
                        piece = roll(frame(p, e) * m, plan.block_lanes * k - lo)
                        value = jnp.where(in_block(k), piece, value)
                    put(x0 + j, value)

        def pair(t):
            unit = unit_of_ref[t]
            code = code_ref[unit]
            x = pl.multiple_of((2 * (t + unit)) * KBLOCK, 16)
            cols = jnp.concatenate(
                [x_ref[pl.ds(x, 256), :], x_ref[pl.ds(x + KBLOCK, 256), :]], axis=1
            )
            y = jnp.dot(w_ref[ev, code], cols, preferred_element_type=f32)
            h = (y + y * jnp.tanh(y)).astype(bf16)
            z = jnp.dot(wo_ref[code], h, preferred_element_type=f32)
            z_ref[2 * t] = z[:, :lanes]
            z_ref[2 * t + 1] = z[:, lanes:]

        group = 4
        assert plan.pairs % group == 0

        def pairs(i, c):
            for s in range(group):
                pair(i * group + s)
            return c

        lax.fori_loop(0, plan.pairs // group, pairs, 0)

        def add(p, e, value):
            total_ref[p, e * OUT : (e + 1) * OUT, :] += value

        for p in range(count):
            z0 = plan.z0[plan.at("mid", p)]

            def mid_out(e, c, p=p, z0=z0):
                total_ref[p, pl.ds(pl.multiple_of(e * OUT, 8), OUT), :] = spread(
                    z0 + e - 2, not_first, not_last
                )
                return c

            lax.fori_loop(REACH, ext - REACH, mid_out, 0, unroll=4)
            for e in range(2, REACH):
                total_ref[p, e * OUT : (e + 1) * OUT, :] = (
                    spread(z0 + e - 2, not_first, not_last) * cuts[0][p]
                )
                d = ext - 1 - e
                total_ref[p, d * OUT : (d + 1) * OUT, :] = (
                    spread(z0 + d - 2, not_first, not_last) * cuts[1][p]
                )
            z0 = plan.z0[plan.at("up", p)]
            for e in range(2, strip):
                terms = (None, None, 0 if e == strip - 1 else None)
                value = spread(z0 + e - 2, not_first, not_last, terms)
                add(p, e, value * (inside if e < REACH else cuts[0][p]))
            z0 = plan.z0[plan.at("down", p)]
            for i in range(strip - 2):
                e = ext - strip + i
                terms = (0 if i == 0 else None, None, None)
                value = spread(z0 + i, not_first, not_last, terms)
                add(p, e, value * (cuts[1][p] if i < RIM else inside))

        for right in (False, True):
            p = last if right else 0
            lo = right_lo if right else left_lo
            outer = right_out if right else left_out
            vertex = count if right else 0
            m_first = block_not_first if right else nothing
            m_last = nothing if right else block_not_last
            top = outer * side_cut(right, flags[0][vertex])
            bottom = outer * side_cut(right, flags[1][vertex])
            z0 = plan.z0[plan.at("right" if right else "left")]
            for j in range(plan.long_rows):
                value = spread(z0 + j, m_first, m_last)
                for k in range(plan.long_blocks):
                    e = plan.long_rows * k + 2 + j
                    if e >= ext - 2:
                        continue
                    m = top if e < REACH else (bottom if e >= ext - REACH else outer)
                    add(p, e, roll(value, lo - plan.block_lanes * k) * m)
            for down in (False, True):
                flag = flags[1 if down else 0][vertex]
                marked = outer * side_cut(right, flag)
                name = ("down" if down else "up") + ("_right" if right else "_left")
                z0 = plan.z0[plan.at(name)]
                first = ext - strip if down else 2
                edge = 0 if down else plan.short_blocks - 1
                others = (block_of != edge).astype(f32)
                for j in range(plan.short_rows):
                    terms = [None, None, None]
                    if down and j == 0:
                        terms[0] = others
                    if not down and j == plan.short_rows - 1:
                        terms[2] = others
                    value = spread(z0 + j, m_first, m_last, terms)
                    for k in range(plan.short_blocks):
                        e = first + plan.short_rows * k + j
                        near = e < ext - REACH if down else e >= REACH
                        add(p, e, roll(value, lo - plan.block_lanes * k) * (marked if near else outer))

        def finish(e, cover):
            at = pl.ds(pl.multiple_of(e * OUT, 8), OUT)
            own = [total_ref[p, at, :] for p in range(count)]
            for p in range(count):
                value = own[p]
                if p + 1 < count:
                    value = value + roll(own[p + 1], side) * (
                        (lane1 >= side) & (lane1 < extent)
                    ).astype(f32)
                if p > 0:
                    value = value + roll(own[p - 1], -side) * (lane1 < 2 * RIM).astype(f32)
                slope = value * cover[p]
                slope_ref[p, at, :] += slope
                where = pl.ds(pl.multiple_of(e * both, 8), OUT)
                frame_ref[p, where, :] += step_size * slope

        for e in range(2, strip):
            finish(e, cover_row[0])
            finish(ext - 1 - e, cover_row[1])

        def finish_mid(e, c):
            finish(e, [cover_mid] * count)
            return c

        lax.fori_loop(strip, ext - strip, finish_mid, 0, unroll=4)
        return carry

    lax.fori_loop(0, 2, evaluation, 0)

    codes = [code_ref[plan.at("mid", p)] for p in range(count)]
    near = iota((side, lanes), 1) < side

    def slopes_of(c):
        at = pl.ds(REACH * OUT + c, side, stride=OUT)
        a, b = slope_ref[0, at, :], slope_ref[1, at, :]
        return jnp.where(near, roll(a, -RIM), roll(b, side - RIM))

    half = fields // 2
    for c in range(half):
        a, b = turned(slopes_of(c), slopes_of(c + half), codes, side)
        out_ref[c] = state_ref[c] + (0.5 * step_size) * a
        out_ref[c + half] = state_ref[c + half] + (0.5 * step_size) * b


def evaluate(orient, corner, state, grid, left, right, up, down, w_state, w_cond, w_out, embeds):
    fields, side, lanes = state.shape
    both = 2 * fields
    plan = Plan(side, lanes)
    sel_state, sel_cond, sel_out = selections(fields)
    smem = pl.BlockSpec(memory_space=pltpu.SMEM)
    vmem = pl.BlockSpec(memory_space=pltpu.VMEM)
    count, ext = plan.count, plan.ext
    return pl.pallas_call(
        functools.partial(main_kernel, plan, orient.shape),
        out_shape=jax.ShapeDtypeStruct(state.shape, f32),
        in_specs=[smem, smem, smem] + [vmem] * 13,
        out_specs=vmem,
        scratch_shapes=[
            pltpu.VMEM((count, ext * both, lanes), f32),
            pltpu.VMEM((count, ext * OUT, lanes), f32),
            pltpu.VMEM((count, ext * OUT, lanes), f32),
            pltpu.VMEM((plan.x_rows * KBLOCK + 256 - KBLOCK, lanes), bf16),
            pltpu.VMEM((plan.z_rows, ZROWS, lanes), f32),
            pltpu.VMEM((2, 4, 256, 256), bf16),
            pltpu.VMEM((4, ZROWS, 256), bf16),
            pltpu.SMEM((len(plan.units),), jnp.int32),
        ],
        name="evaluate",
    )(
        jnp.asarray(np.array(plan.unit_of, np.int32)),
        orient,
        corner,
        state,
        grid,
        left,
        right,
        up,
        down,
        w_state,
        w_cond,
        w_out,
        embeds,
        jnp.asarray(sel_state, bf16),
        jnp.asarray(sel_cond, bf16),
        jnp.asarray(sel_out, bf16),
    )


def shifted(value, axis, steps):
    count = lax.axis_size(axis)
    return lax.ppermute(value, axis, [(i, (i + steps) % count) for i in range(count)])


def local(
    noisy_state,
    conditioning,
    orient,
    corner_points,
    w_state,
    w_cond,
    w_out,
    embed_first,
    embed_second,
):
    both = 2 * noisy_state.shape[0]
    grid, to_left, to_right = prepare(orient, noisy_state, conditioning)
    left = shifted(to_right, "tile", 1)
    right = shifted(to_left, "tile", -1)
    to_up, to_down = edges(grid, left, right, both)
    up = shifted(to_down, "face", 1)
    down = shifted(to_up, "face", -1)
    embeds = jnp.stack([embed_first, embed_second])
    return evaluate(
        orient, corner_points, noisy_state, grid, left, right, up, down, w_state, w_cond, w_out, embeds
    )


def solution(mesh):
    return jax.shard_map(
        local,
        mesh=mesh,
        in_specs=(
            P("groups", "face", "tile"),
            P("groups", "face", "tile"),
            P(),
            P(),
            P(),
            P(),
            P(),
            P(),
            P(),
        ),
        out_specs=P("groups", "face", "tile"),
        check_vma=False,
    )
```
